32 devices in a mesh: grp: 2 (over y), dp: 16 (over z, x, core).
Axes of the slice: x: 2, y: 2, z: 4, core: 2. Of those that a mesh axis runs over, the one named last changes fastest.
Arguments:
- hidden_in: bfloat16 [2, 64, 4096], P(None, ('grp', 'dp')), parts along dimension 1, may hold values from -6 to 6
- norm_gain: float32 [4096], replicated, may hold values from 0.1 to 1.9
- queries: bfloat16 [2, 64, 4096], P(None, ('grp', 'dp')), parts along dimension 1, may hold values from -72 to 72
- new_keys: bfloat16 [2, 64, 1024], P(None, ('grp', 'dp')), parts along dimension 1, may hold values from -9 to 9
- new_values: bfloat16 [2, 64, 1024], P(None, ('grp', 'dp')), parts along dimension 1, may hold values from -6 to 6
- cache_keys: bfloat16 [64, 384, 1024], P(('grp', 'dp')), parts along dimension 0, may hold values from -9 to 9
- cache_values: bfloat16 [64, 384, 1024], P(('grp', 'dp')), parts along dimension 0, may hold values from -6 to 6
- lengths: int32 [64], P(('grp', 'dp')), parts along dimension 0, may hold values from 1 to 384
- routes: int32 [2, 64, 2], P(None, ('grp', 'dp')), parts along dimension 1, may hold values from 0 to 3, all different within a row; in each aligned block of 2 rows (0 to 1, 2 to 3, ..., all dimensions but the last counted through in order) at most 2 rows name the same one
- gate_logits: float32 [2, 64, 2], P(None, ('grp', 'dp')), parts along dimension 1, may hold values from -6 to 6
- w_gate: bfloat16 [28672, 4096], P('dp'), may hold values from -0.09375 to 0.09375
- w_up: bfloat16 [28672, 4096], P('dp'), may hold values from -0.09375 to 0.09375
- w_down: bfloat16 [28672, 4096], P('dp'), may hold values from -0.0625 to 0.0625
Outputs:
- hidden_out: bfloat16 [2, 64, 4096], P(None, ('grp', 'dp')), parts along dimension 1
The draws below stay inside these ranges and needn't reach their ends.
There are 2 independent parts, one for each index of `grp`. The reference program is written for one: setup_inputs(seed, part) draws one part's arguments, and reference() takes and returns one part's arrays. A program takes and returns all parts, laid end to end along the dimension named above; an argument that names none is the same for every part. Nothing has to cross between parts.
Inputs may be any that keep to these rules, and one draw needn't show every extreme that they name: `routes`: each token names 2 different experts. Among the 2 tokens of one device at one decoded position no expert is named more than 2 times, a bound that some block reaches.
All inputs are finite; a program needn't handle non-finite values.
Results may differ from the reference program's by a relative error of at most 0.0055.
Values may be sent and summed in bfloat16 or wider, within the bound.
A program may use at most 192 MiB of HBM per device.

```python
import math
import jax
import jax.numpy as jnp
import numpy as np
from jax import lax

D = 4096
HEADS = 32
KV_HEADS = 8
HEAD_DIM = 128
TOP = 2
EXPERTS = 4
FFW = 7168
NEW = 2
DOC_DEV = 2
CACHE = 384
DOCS = 32
GROUP = 4
KV_WIDTH = 1024
CAP = 2


def key_fields(key):
    cached = jnp.clip(jax.random.normal(jax.random.fold_in(key, 101), (DOCS, CACHE, KV_HEADS * HEAD_DIM), jnp.float32), -5.0, 5.0)
    fresh = jnp.clip(jax.random.normal(jax.random.fold_in(key, 102), (NEW, DOCS, KV_HEADS * HEAD_DIM), jnp.float32), -5.0, 5.0)
    return (cached, fresh)


def draw_cache_keys(key, part):
    cached, fresh = key_fields(key)
    return cached.astype(jnp.bfloat16)


def draw_new_keys(key, part):
    cached, fresh = key_fields(key)
    return fresh.astype(jnp.bfloat16)


def draw_queries(key, part):
    drawn = jnp.clip(jax.random.normal(jax.random.fold_in(key, 104), (NEW, DOCS, HEADS * HEAD_DIM), jnp.float32), -5.0, 5.0)
    return drawn.astype(jnp.bfloat16)


def touch_ends(values, own_key, low, high):
    shape = values.shape
    index_at = [jax.random.randint(jax.random.fold_in(own_key, axis), (), 0, shape[axis]) for axis in range(len(shape))]
    values = values.at[tuple(index_at)].set(low)
    longest = shape.index(max(shape))
    index_at[longest] = (index_at[longest] + 1) % shape[longest]
    return values.at[tuple(index_at)].set(high)


def steps_of(key, extent, shards, low, top_value):
    def one(axis_at, parts):
        steps = jax.random.uniform(jax.random.fold_in(jax.random.fold_in(key, 6), axis_at), (parts,), jnp.float32, low / len(shards), top_value / len(shards))
        return jnp.repeat(jnp.exp(steps), extent[axis_at] // parts).reshape((-1,) + (1,) * (len(extent) - axis_at - 1))

    loudness = one(*shards[0])
    for cut in shards[1:]:
        loudness = loudness * one(*cut)
    return loudness


def routed_block(own_key, own, number, rows, amount, top, most, lean):
    sequence = jax.random.permutation(own_key, amount)
    crowded, common = load_shares(amount, rows * top, most, lean, True), load_shares(amount, rows * top, most, lean, False)
    places = jnp.arange(amount)

    def named(sizes, turn):
        used = int((sizes > 0).sum())
        fixed = max(1, used // 4)
        passed = fixed + (places - fixed + turn * (used - fixed)) % max(1, amount - fixed)
        return jnp.zeros((amount,), jnp.int32).at[sequence[jnp.where(places < fixed, places, passed)]].set(jnp.asarray(sizes, jnp.int32))

    sizes = jnp.where(number % 4 == 0, named(crowded, number // 4), named(common, number - number // 4 - 1))
    mixed = jax.random.permutation(jax.random.fold_in(own, 3), amount)
    source_of, taker = mixed[0:amount // 2 * 2:2], mixed[1:amount // 2 * 2:2]
    margin = jnp.minimum(sizes[source_of] - 1, most - sizes[taker]) // 2
    margin = jnp.where((source_of == sequence[0]) | (taker == sequence[0]) | (sizes[taker] == 0), 0, jnp.maximum(margin, 0))
    passed = jax.random.randint(jax.random.fold_in(own, 4), (amount // 2,), 0, 1 << 20) % (margin + 1)
    sizes = sizes.at[source_of].add(-passed).at[taker].add(passed)
    labels = jnp.searchsorted(jnp.cumsum(sizes), jnp.arange(rows * top), side="right").astype(jnp.int32)
    table = labels.reshape(top, rows).T
    table = table[jax.random.permutation(jax.random.fold_in(own, 1), rows)]
    turn = jax.random.randint(jax.random.fold_in(own, 2), (rows, 1), 0, top)
    return jnp.take_along_axis(table, (jnp.arange(top)[None, :] + turn) % top, axis=1)


def load_shares(amount, total, limit, lean, full):
    weights = [(1 << 20) // math.isqrt(grade ** lean) + 1 for grade in range(1, amount + 1)]
    largest = limit if full else min(limit, max(-(-total // amount), total * weights[0] // sum(weights)))
    least = 1 if total - largest >= amount - 1 else 0
    holding, spare = [largest] + [least] * (amount - 1), total - largest - least * (amount - 1)
    while spare > 0:
        free = [i for i in range(1, amount) if holding[i] < largest] or [i for i in range(1, amount) if holding[i] < limit]
        whole, budget = sum([weights[i] for i in free]), spare
        for i in free:
            more = min(limit - holding[i], max(1, budget * weights[i] // whole), spare)
            holding[i] = holding[i] + more
            spare = spare - more
    return np.array(holding)


def gaussian(key, dims, scale, most, shards=(), kind=jnp.bfloat16):
    values = jax.random.normal(key, dims, jnp.float32) * scale
    if len(shards) > 0:
        values = steps_of(key, dims, shards, -0.22, 0.18) * values
    return jnp.clip(values, min=-most, max=most).astype(kind)


def setup_inputs(seed: int = 0, part: int = 0) -> dict:
    arg_keys = jax.random.split(jax.random.key(seed), 14)
    part_keys = jax.random.split(jax.random.fold_in(arg_keys[13], part), 14)
    hidden_in = gaussian(part_keys[0], (NEW, DOCS, D), 1.0, 6.0, ((1, 16),))
    norm_gain = jnp.clip(1.0 + 0.18 * jax.random.normal(arg_keys[1], (D,), jnp.float32), 0.1, 1.9)
    queries = draw_queries(jax.random.fold_in(jax.random.fold_in(arg_keys[13], part), 71), part)
    new_keys = draw_new_keys(jax.random.fold_in(jax.random.fold_in(arg_keys[13], part), 71), part)
    new_values = gaussian(part_keys[4], (NEW, DOCS, KV_WIDTH), 1.0, 6.0, ((1, 16),))
    cache_keys = draw_cache_keys(jax.random.fold_in(jax.random.fold_in(arg_keys[13], part), 71), part)
    cache_values = gaussian(part_keys[6], (DOCS, CACHE, KV_WIDTH), 1.0, 6.0, ((0, 16),))
    lengths = touch_ends(jax.random.randint(part_keys[7], (DOCS,), 1, CACHE + 1), jax.random.fold_in(part_keys[7], 1), 1, CACHE).astype(jnp.int32)
    routes_keys = jax.random.split(jax.random.fold_in(part_keys[8], 1), NEW * DOCS // DOC_DEV)
    routes_turns = jax.random.permutation(jax.random.fold_in(part_keys[8], 3), NEW * DOCS // DOC_DEV)
    routes = jax.vmap(lambda own, number: routed_block(jax.random.fold_in(part_keys[8], 2), own, number, DOC_DEV, EXPERTS, TOP, CAP, 2))(routes_keys, routes_turns).reshape((NEW, DOCS, TOP))
    gate_logits = gaussian(part_keys[9], (NEW, DOCS, TOP), 1.5, 6.0, ((1, 16),), jnp.float32)
    w_gate = gaussian(arg_keys[10], (EXPERTS * FFW, D), D ** -0.5, 0.09375, ((0, 16),))
    w_up = gaussian(arg_keys[11], (EXPERTS * FFW, D), D ** -0.5, 0.09375, ((0, 16),))
    w_down = gaussian(arg_keys[12], (EXPERTS * FFW, D), FFW ** -0.5, 0.0625, ((0, 16),))
    return {"hidden_in": hidden_in, "norm_gain": norm_gain, "queries": queries, "new_keys": new_keys, "new_values": new_values, "cache_keys": cache_keys, "cache_values": cache_values, "lengths": lengths, "routes": routes, "gate_logits": gate_logits, "w_gate": w_gate, "w_up": w_up, "w_down": w_down}


def attend(queries, new_keys, new_values, cache_keys, cache_values, lengths):
    docs = queries.shape[1]
    cache_len = cache_keys.shape[1]
    score_scale = HEAD_DIM ** (-0.5)
    query_heads = queries.astype(jnp.float32).reshape(NEW, docs, KV_HEADS, GROUP, HEAD_DIM)
    keys_cache = cache_keys.astype(jnp.float32).reshape(docs, cache_len, KV_HEADS, HEAD_DIM)
    vals_cache = cache_values.astype(jnp.float32).reshape(docs, cache_len, KV_HEADS, HEAD_DIM)
    keys_fresh = new_keys.astype(jnp.float32).reshape(NEW, docs, KV_HEADS, HEAD_DIM)
    vals_fresh = new_values.astype(jnp.float32).reshape(NEW, docs, KV_HEADS, HEAD_DIM)
    scores_cache = jnp.einsum('tdhgc,dshc->tdhgs', query_heads, keys_cache) * score_scale
    scores_fresh = jnp.einsum('tdhgc,udhc->tdhgu', query_heads, keys_fresh) * score_scale
    positions = jnp.arange(cache_len, dtype=jnp.int32)
    in_range = positions[None, :] < lengths[:, None]
    scores_cache = jnp.where(in_range[None, :, None, None, :], scores_cache, -1e+30)
    order = jnp.arange(NEW, dtype=jnp.int32)
    causal = order[None, :] <= order[:, None]
    scores_fresh = jnp.where(causal[:, None, None, None, :], scores_fresh, -1e+30)
    largest = jnp.maximum(lax.optimization_barrier(jnp.max(scores_cache, -1, keepdims=True)), lax.optimization_barrier(jnp.max(scores_fresh, -1, keepdims=True)))
    exp_cache = jnp.exp(scores_cache - largest)
    exp_fresh = jnp.exp(scores_fresh - largest)
    total = lax.optimization_barrier(jnp.sum(exp_cache, -1, keepdims=True)) + lax.optimization_barrier(jnp.sum(exp_fresh, -1, keepdims=True))
    probs_cache = (exp_cache / total).astype(jnp.bfloat16).astype(jnp.float32)
    probs_fresh = (exp_fresh / total).astype(jnp.bfloat16).astype(jnp.float32)
    context = jnp.einsum('tdhgs,dshc->tdhgc', probs_cache, vals_cache)
    context = context + jnp.einsum('tdhgu,udhc->tdhgc', probs_fresh, vals_fresh)
    return context.reshape(NEW, docs, HEADS * HEAD_DIM)

def reference(hidden_in, norm_gain, queries, new_keys, new_values, cache_keys, cache_values, lengths, routes, gate_logits, w_gate, w_up, w_down):
    context = attend(queries, new_keys, new_values, cache_keys, cache_values, lengths)
    carried = hidden_in.astype(jnp.float32) + context
    normed = (carried * lax.rsqrt(lax.optimization_barrier(jnp.mean(carried * carried, -1, keepdims=True)) + 1e-05) * norm_gain).astype(jnp.bfloat16)
    flat_rows = normed.reshape(NEW * DOCS, D)
    flat_routes = routes.reshape(NEW * DOCS, TOP)
    flat_logits = gate_logits.reshape(NEW * DOCS, TOP)
    top_share = jax.nn.sigmoid(flat_logits[:, 0] - flat_logits[:, 1])
    shares = jnp.stack([top_share, 1.0 - top_share], axis=1)
    result = carried.reshape(NEW * DOCS, D)
    for expert in range(EXPERTS):
        weight_rows = lax.optimization_barrier(jnp.sum(shares * (flat_routes == expert).astype(jnp.float32), axis=1))
        gate_block = w_gate[expert * FFW:(expert + 1) * FFW]
        up_block = w_up[expert * FFW:(expert + 1) * FFW]
        down_block = w_down[expert * FFW:(expert + 1) * FFW]
        gate_val = lax.dot_general(flat_rows, gate_block, (((1,), (1,)), ((), ())), preferred_element_type=jnp.float32)
        up_val = lax.dot_general(flat_rows, up_block, (((1,), (1,)), ((), ())), preferred_element_type=jnp.float32)
        act = (jax.nn.silu(gate_val) * up_val).astype(jnp.bfloat16)
        expert_out = jnp.dot(act, down_block, preferred_element_type=jnp.float32)
        result = result + weight_rows[:, None] * expert_out
    return result.reshape(NEW, DOCS, D).astype(jnp.bfloat16)
```

```python
import functools

import jax
import jax.numpy as jnp
from jax import lax
from jax.experimental import pallas as pl
from jax.experimental.pallas import tpu as pltpu
from jax.sharding import PartitionSpec as P

HEAD_DIM = 128
EXPERTS = 4
PAD = 16
MESH = pl.DeviceIdType.MESH
F32 = jnp.float32
BF16 = jnp.bfloat16
NEG = -1e30
PARTS = ((2, False), (1, False), (1, True), (1, True), (1, True), (1, True), (1, True))
ROWS_BY_ROWS = (((1,), (1,)), ((), ()))
COLS_BY_ROWS = (((0,), (0,)), ((), ()))


def kernel(
    n,
    pieces,
    parts,
    lengths_hbm,
    routes_hbm,
    logits_hbm,
    hidden_hbm,
    gain_hbm,
    q_hbm,
    nk_hbm,
    nv_hbm,
    ck_hbm,
    cv_hbm,
    wg_hbm,
    wu_hbm,
    wd_hbm,
    out_ref,
    lengths_ref,
    routes_ref,
    logits_ref,
    hidden_ref,
    gain_ref,
    q_ref,
    nk_ref,
    nv_ref,
    kvbuf,
    wgu,
    wd,
    qs,
    bias,
    carried,
    blocks,
    xs,
    xb,
    ssq,
    acc_g,
    acc_u,
    act,
    part,
    s1,
    r1,
    s2,
    r2,
    s3,
    r3,
    s4,
    r4,
    sem_in,
    sem_kv,
    sem_gu,
    sem_d,
    sem_a,
    sem_c,
    sem_r,
    sem_s,
):
    new, docs, width = hidden_ref.shape
    tokens = new * docs
    cache_len, kv_width = ck_hbm.shape[1], ck_hbm.shape[2]
    kv_heads = kv_width // HEAD_DIM
    group = width // kv_width
    hidden = wg_hbm.shape[0]
    pair = 2
    nc = kv_heads // pair
    ck = width // nc
    nk = len(parts)
    relayed = [k for k, (_, _, direct) in enumerate(parts) if not direct]
    straight = [k for k, (_, _, direct) in enumerate(parts) if direct]
    quads = n // 4
    rows = n * tokens
    half = rows // 2
    score_scale = HEAD_DIM ** (-0.5)

    grp, me = lax.axis_index("grp"), lax.axis_index("dp")
    core = lax.rem(me, 2)
    xbit = lax.rem(me // 2, 2)
    quad = me // 4
    core_dev = (grp, me + 1 - 2 * core)
    x_dev = (grp, me + 2 - 4 * xbit)

    def quad_dev(d):
        return (grp, lax.rem(quad + d, quads) * 4 + lax.rem(me, 4))

    def diagonal_dev(d):
        return (grp, lax.rem(quad + d, quads) * 4 + lax.rem(me, 4) + 2 - 4 * xbit)

    barrier = pltpu.get_barrier_semaphore()
    order = [d for i in range(quads // 2, 0, -1) for d in dict.fromkeys([i, quads - i])]
    chips = [dev(d) for d in order for dev in (diagonal_dev, quad_dev)] + [x_dev]
    for dev in chips + [core_dev]:
        pl.semaphore_signal(barrier, inc=1, device_id=dev, device_id_type=MESH)

    smalls = [
        (q_hbm, q_ref),
        (nk_hbm, nk_ref),
        (nv_hbm, nv_ref),
        (lengths_hbm, lengths_ref),
        (hidden_hbm, hidden_ref),
        (gain_hbm, gain_ref),
        (routes_hbm, routes_ref),
        (logits_hbm, logits_ref),
    ]
    small_copies = [
        pltpu.make_async_copy(src, dst, sem_in.at[i]) for i, (src, dst) in enumerate(smalls)
    ]

    def lanes_of(c):
        return pl.ds(c * pair * HEAD_DIM, pair * HEAD_DIM)

    def cache_rows(c):
        return kvbuf.at[:, :, pl.ds(0, cache_len), lanes_of(c)]

    def cache_copies(c):
        return [
            pltpu.make_async_copy(src.at[:, :, lanes_of(c)], cache_rows(c).at[i], sem_kv.at[c])
            for i, src in enumerate((ck_hbm, cv_hbm))
        ]

    for copy in small_copies[:5] + cache_copies(0) + small_copies[5:]:
        copy.start()
    for c in range(1, nc):
        for copy in cache_copies(c):
            copy.start()

    def start_weights():
        for p, (at, size, _) in enumerate(pieces):
            for i, src in enumerate((wg_hbm, wu_hbm)):
                lanes = pl.ds(at, size)
                pltpu.make_async_copy(src.at[:, lanes], wgu.at[i, :, lanes], sem_gu.at[p]).start()
        pltpu.make_async_copy(wd_hbm, wd, sem_d.at[0]).start()

    with jax.named_scope("inwait"):
        for copy in small_copies[:5]:
            copy.wait()
    for t in range(new):
        q32 = q_ref[t].astype(F32)
        for head in range(kv_heads * group):
            qs[head * tokens + t * docs : head * tokens + (t + 1) * docs, :] = q32[
                :, head * HEAD_DIM : (head + 1) * HEAD_DIM
            ]
        carried[t * docs : (t + 1) * docs, :] = hidden_ref[t].astype(F32)
    extra = lax.broadcasted_iota(jnp.int32, (PAD, kv_width), 0)
    for i, src in enumerate((nk_ref, nv_ref)):
        for d in range(docs):
            value = jnp.zeros((PAD, kv_width), F32)
            for u in range(new):
                value = jnp.where(extra == u, src[u, d : d + 1].astype(F32), value)
            kvbuf[i, d, cache_len : cache_len + PAD, :] = value.astype(BF16)
    prow = pair * group * tokens
    row = lax.broadcasted_iota(jnp.int32, (prow, cache_len + PAD), 0)
    col = lax.broadcasted_iota(jnp.int32, (prow, cache_len + PAD), 1)
    row_doc = lax.rem(row, docs)
    row_new = lax.rem(row, tokens) // docs
    limit = jnp.zeros_like(row)
    for d in range(docs):
        limit = jnp.where(row_doc == d, lengths_ref[d], limit)
    keep = (col < limit) | ((col >= cache_len) & (col - cache_len <= row_new))
    keep = jnp.logical_and(keep, (col < cache_len) | (col < cache_len + new))
    bias[...] = jnp.where(keep, 0.0, NEG)

    def block_copy(p, index, count, send_sem, recv_sem, dev):
        ref = blocks.at[pl.ds(index, count), :, pl.ds(pieces[p][0], pieces[p][1])]
        return pltpu.make_async_remote_copy(
            src_ref=ref,
            dst_ref=ref,
            send_sem=sem_s.at[send_sem],
            recv_sem=recv_sem.at[p],
            device_id=dev,
            device_id_type=MESH,
        )

    mine = (core * 2 + xbit) * quads + quad

    def core_copy(p, z):
        index = lax.rem(core + z, 2) * 2 * quads
        return block_copy(p, index, 2 * quads, 1, sem_c, core_dev)

    def scores_of(c):
        zeros = jnp.zeros((group * tokens, HEAD_DIM), F32)
        lines = []
        for i in range(pair):
            h = c * pair + i
            q = qs[h * group * tokens : (h + 1) * group * tokens, :]
            lines.append(jnp.concatenate([zeros] * i + [q] + [zeros] * (pair - 1 - i), axis=1))
        q = jnp.concatenate(lines, axis=0).astype(BF16)
        lanes = slice(c * pair * HEAD_DIM, (c + 1) * pair * HEAD_DIM)
        value = None
        for d in range(docs):
            s = lax.dot_general(
                q, kvbuf[0, d, :, lanes], ROWS_BY_ROWS, preferred_element_type=F32
            )
            value = s if d == 0 else jnp.where(row_doc == d, s, value)
        return value

    def context_of(c, value):
        value = value * score_scale + bias[...]
        e = jnp.exp(value - jnp.max(value, axis=1, keepdims=True))
        p = e * (1.0 / jnp.sum(e, axis=1, keepdims=True))
        lanes = slice(c * pair * HEAD_DIM, (c + 1) * pair * HEAD_DIM)
        result = None
        for d in range(docs):
            r = jnp.dot(
                jnp.where(row_doc == d, p, 0.0).astype(BF16),
                kvbuf[1, d, :, lanes],
                preferred_element_type=F32,
            )
            result = r if d == 0 else result + r
        pieces = []
        for i in range(pair):
            for g in range(group):
                at = (i * group + g) * tokens
                pieces.append(result[at : at + tokens, i * HEAD_DIM : (i + 1) * HEAD_DIM])
        return jnp.concatenate(pieces, axis=1)

    def wait_cache(c):
        with jax.named_scope(f"kv{c}"):
            pltpu.make_async_copy(cache_rows(c), cache_rows(c), sem_kv.at[c]).wait()

    def attend(c, value):
        with jax.named_scope(f"attn{c}"):
            lanes = slice(c * ck, (c + 1) * ck)
            car = carried[:, lanes] + context_of(c, value)
            carried[:, lanes] = car
            blocks[mine, :, lanes] = car.astype(BF16)

    def send_chunk(c):
        for p, (_, _, chunk) in enumerate(pieces):
            if chunk == c:
                for dev in chips:
                    block_copy(p, mine, 1, 0, sem_a, dev).start()

    wait_cache(0)
    attend(0, scores_of(0))
    with jax.named_scope("bar"):
        pl.semaphore_wait(barrier, 2 * quads)
    send_chunk(0)
    for c in range(1, nc):
        wait_cache(c)
    start_weights()
    with jax.named_scope("scores1"):
        values = [scores_of(c) for c in range(1, nc)]
    for c in range(1, nc):
        attend(c, values[c - 1])
        send_chunk(c)
    for copy in small_copies[5:]:
        copy.wait()

    def forward(p):
        with jax.named_scope(f"A{p}"):
            block_copy(p, 0, 2 * quads - 1, 0, sem_a, core_dev).wait_recv()
            core_copy(p, 0).start()

    def gather(p):
        at, size, _ = pieces[p]
        lanes = slice(at, at + size)
        with jax.named_scope(f"C{p}"):
            core_copy(p, 1).wait_recv()
        for b in range(n):
            xs[b * tokens : (b + 1) * tokens, 0:size] = blocks[b, :, lanes].astype(F32)
        value = xs[:, 0:size]
        square = value * value
        total = square[:, 0:HEAD_DIM]
        for i in range(1, size // HEAD_DIM):
            total = total + square[:, i * HEAD_DIM : (i + 1) * HEAD_DIM]
        ssq[...] = total if p == 0 else ssq[...] + total
        xb[:, lanes] = (value * gain_ref[:, lanes]).astype(BF16)

    nh = 2
    hc = hidden // nh

    def gate_up(p, j, scale):
        rows_at = slice(j * hc, (j + 1) * hc)
        lanes = slice(pieces[p][0], pieces[p][0] + pieces[p][1])
        x = xb[:, lanes]
        g = lax.dot_general(wgu[0, rows_at, lanes], x, ROWS_BY_ROWS, preferred_element_type=F32)
        u = lax.dot_general(wgu[1, rows_at, lanes], x, ROWS_BY_ROWS, preferred_element_type=F32)
        if p > 0:
            g = g + acc_g[rows_at, :]
            u = u + acc_u[rows_at, :]
        if p < len(pieces) - 1:
            acc_g[rows_at, :] = g
            acc_u[rows_at, :] = u
        else:
            g = g * scale
            act[rows_at, :] = (g * jax.nn.sigmoid(g) * (u * scale)).astype(BF16)

    forward(0)
    for p, (at, size, _) in enumerate(pieces):
        gather(p)
        scale = None
        if p == len(pieces) - 1:
            total = jnp.sum(jnp.transpose(ssq[...]), axis=0, keepdims=True)
            scale = lax.rsqrt(total / width + 1e-05)
        with jax.named_scope(f"guwait{p}"):
            ref = wgu.at[:, :, pl.ds(at, size)]
            pltpu.make_async_copy(ref, ref, sem_gu.at[p]).wait()
        for j in range(nh):
            with jax.named_scope(f"gu{p}"):
                gate_up(p, j, scale)
            if j == 0 and p < len(pieces) - 1:
                forward(p + 1)

    def pair_copy(src, dst, stage, k, dev):
        return pltpu.make_async_remote_copy(
            src_ref=src,
            dst_ref=dst,
            send_sem=sem_s.at[2 + stage],
            recv_sem=sem_r.at[min(stage, 2), k],
            device_id=dev,
            device_id_type=MESH,
        )

    def lanes_at(k):
        return pl.ds(parts[k][0], parts[k][1])

    copy_1 = [
        pair_copy(s1.at[1 - core, :, lanes_at(k)], r1.at[:, lanes_at(k)], 0, k, core_dev)
        for k in range(nk)
    ]
    copy_2 = {
        k: pair_copy(s2.at[1 - xbit, :, lanes_at(k)], r2.at[:, lanes_at(k)], 1, k, x_dev)
        for k in relayed
    }
    others = pl.ds(0, quads - 1)
    rest = pl.ds(0, 2 * quads - 1)

    def sends_3(k):
        lanes = lanes_at(k)
        return [
            pair_copy(
                s3.at[lax.rem(quad + d, quads), :, lanes], r3.at[quad, :, lanes], 2, k, quad_dev(d)
            )
            for d in range(1, quads)
        ]

    def sends_4(k):
        lanes = lanes_at(k)
        here = r4.at[xbit * quads + quad, :, lanes]
        copies = []
        for d in order:
            to = lax.rem(quad + d, quads)
            for x, dev in ((1 - xbit, diagonal_dev(d)), (xbit, quad_dev(d))):
                copies.append(pair_copy(s4.at[x * quads + to, :, lanes], here, 3, k, dev))
        copies.append(pair_copy(s4.at[(1 - xbit) * quads + quad, :, lanes], here, 3, k, x_dev))
        return copies

    def start_1(k):
        at, size, _ = parts[k]
        lanes = slice(at, at + size)
        with jax.named_scope(f"down{k}"):
            value = lax.dot_general(act[...], wd[:, lanes], COLS_BY_ROWS, preferred_element_type=F32)
            s1[0, :, lanes] = value[:half].astype(BF16)
            s1[1, :, lanes] = value[half:].astype(BF16)
        copy_1[k].start()

    def start_2(k):
        at, size, direct = parts[k]
        lanes = slice(at, at + size)
        with jax.named_scope(f"r1wait{k}"):
            copy_1[k].wait_recv()
        value = s1[core, :, lanes].astype(F32) + r1[:, lanes].astype(F32)
        if direct:
            for i in range(2 * quads):
                s4[i, :, lanes] = value[i * tokens : (i + 1) * tokens].astype(BF16)
            own = xbit * quads + quad
            r4[own, :, lanes] = s4[own, :, lanes]
            for copy in sends_4(k):
                copy.start()
        else:
            value = value.astype(BF16)
            s2[0, :, lanes] = value[: half // 2]
            s2[1, :, lanes] = value[half // 2 :]
            copy_2[k].start()

    def start_3(k):
        at, size, _ = parts[k]
        lanes = slice(at, at + size)
        with jax.named_scope(f"r2wait{k}"):
            copy_2[k].wait_recv()
        part[:, 0:size] = s2[xbit, :, lanes].astype(F32) + r2[:, lanes].astype(F32)
        for q in range(quads):
            s3[q, :, lanes] = part[q * tokens : (q + 1) * tokens, 0:size].astype(BF16)
        r3[quad, :, lanes] = s3[quad, :, lanes]
        for copy in sends_3(k):
            copy.start()

    token = lax.broadcasted_iota(jnp.int32, (tokens, 1), 0)
    margin = jnp.zeros((tokens, 1), F32)
    first = jnp.zeros((tokens, 1), jnp.int32)
    second = jnp.zeros((tokens, 1), jnp.int32)
    for t in range(new):
        for d in range(docs):
            here = token == t * docs + d
            margin = jnp.where(here, logits_ref[t, d, 0] - logits_ref[t, d, 1], margin)
            first = jnp.where(here, routes_ref[t, d, 0], first)
            second = jnp.where(here, routes_ref[t, d, 1], second)
    share_a = jax.nn.sigmoid(margin)
    share_b = 1.0 - share_a
    share = [
        jnp.where(first == e, share_a, 0.0) + jnp.where(second == e, share_b, 0.0)
        for e in range(EXPERTS)
    ]

    def finish(k):
        at, size, direct = parts[k]
        lanes = slice(at, at + size)
        with jax.named_scope(f"r3wait{k}"):
            if direct:
                pair_copy(
                    s4.at[rest, :, lanes_at(k)], r4.at[rest, :, lanes_at(k)], 3, k, core_dev
                ).wait_recv()
            else:
                pair_copy(
                    s3.at[others, :, lanes_at(k)], r3.at[others, :, lanes_at(k)], 2, k, core_dev
                ).wait_recv()
        acc = carried[:, lanes]
        per = quads // EXPERTS
        for e in range(EXPERTS):
            if direct:
                got = [r4[x * quads + e * per + i, :, lanes] for x in range(2) for i in range(per)]
            else:
                got = [r3[e * per + i, :, lanes] for i in range(per)]
            value = got[0].astype(F32)
            for more in got[1:]:
                value = value + more.astype(F32)
            acc = acc + share[e] * value
        for t in range(new):
            out_ref[t, :, lanes] = acc[t * docs : (t + 1) * docs].astype(out_ref.dtype)

    with jax.named_scope("dwait"):
        pltpu.make_async_copy(wd_hbm, wd, sem_d.at[0]).wait()
    lag = min(2, nk)
    for k in range(nk):
        start_1(k)
        if k >= lag:
            start_2(k - lag)
    for k in range(nk - lag, nk):
        start_2(k)
    for k in relayed:
        start_3(k)
    for k in range(nk):
        finish(k)

    def span(indices):
        at = parts[indices[0]][0]
        return pl.ds(at, parts[indices[-1]][0] + parts[indices[-1]][1] - at)

    with jax.named_scope("sends"):
        sent = [blocks.at[rest], blocks.at[pl.ds(0, 2 * quads)], r1]
        sent += [r2.at[:, span(relayed)], s3.at[others, :, span(relayed)]] if relayed else [None] * 2
        sent += [s4.at[rest, :, span(straight)]] if straight else []
        for i, ref in enumerate(sent):
            if ref is None:
                continue
            pltpu.make_async_remote_copy(
                src_ref=ref,
                dst_ref=ref,
                send_sem=sem_s.at[i],
                recv_sem=sem_s.at[i],
                device_id=core_dev,
                device_id_type=MESH,
            ).wait_send()


def per_device(
    hidden_in,
    norm_gain,
    queries,
    new_keys,
    new_values,
    cache_keys,
    cache_values,
    lengths,
    routes,
    gate_logits,
    w_gate,
    w_up,
    w_down,
):
    n = lax.axis_size("dp")
    new, docs, width = hidden_in.shape
    tokens = new * docs
    rows = n * tokens
    hidden = w_gate.shape[0]
    cache_len, kv_width = cache_keys.shape[1:]
    kv_heads = kv_width // HEAD_DIM
    group = width // kv_width
    quads = n // 4
    chunk = 2 * HEAD_DIM * group
    pieces = [(0, chunk // 2, 0), (chunk // 2, chunk // 2, 0)]
    pieces += [(c * chunk, chunk, c) for c in range(1, width // chunk)]
    parts, at = [], 0
    for size, direct in PARTS:
        parts.append((at * width // 8, size * width // 8, direct))
        at += size
    vmem = pl.BlockSpec(memory_space=pltpu.VMEM)
    hbm = pl.BlockSpec(memory_space=pl.ANY)
    dma = pltpu.SemaphoreType.DMA
    return pl.pallas_call(
        functools.partial(kernel, n, pieces, parts),
        out_shape=pltpu.VMEM(hidden_in.shape, BF16),
        in_specs=[hbm] * 13,
        out_specs=vmem,
        scratch_shapes=[
            pltpu.SMEM(lengths.shape, jnp.int32),
            pltpu.SMEM(routes.shape, jnp.int32),
            pltpu.SMEM(gate_logits.shape, F32),
            pltpu.VMEM(hidden_in.shape, BF16),
            pltpu.VMEM((1, width), F32),
            pltpu.VMEM(queries.shape, BF16),
            pltpu.VMEM(new_keys.shape, BF16),
            pltpu.VMEM(new_values.shape, BF16),
            pltpu.VMEM((2, docs, cache_len + PAD, kv_width), BF16),
            pltpu.VMEM((2, hidden, width), BF16),
            pltpu.VMEM((hidden, width), BF16),
            pltpu.VMEM((kv_heads * group * tokens, HEAD_DIM), F32),
            pltpu.VMEM((2 * group * tokens, cache_len + PAD), F32),
            pltpu.VMEM((tokens, width), F32),
            pltpu.VMEM((n, tokens, width), BF16),
            pltpu.VMEM((rows, chunk), F32),
            pltpu.VMEM((rows, width), BF16),
            pltpu.VMEM((rows, HEAD_DIM), F32),
            pltpu.VMEM((hidden, rows), F32),
            pltpu.VMEM((hidden, rows), F32),
            pltpu.VMEM((hidden, rows), BF16),
            pltpu.VMEM((rows // 4, chunk), F32),
            pltpu.VMEM((2, rows // 2, width), BF16),
            pltpu.VMEM((rows // 2, width), BF16),
            pltpu.VMEM((2, rows // 4, width), BF16),
            pltpu.VMEM((rows // 4, width), BF16),
            pltpu.VMEM((quads, tokens, width), BF16),
            pltpu.VMEM((quads, tokens, width), BF16),
            pltpu.VMEM((2 * quads, tokens, width), BF16),
            pltpu.VMEM((2 * quads, tokens, width), BF16),
            dma((8,)),
            dma((kv_heads // 2,)),
            dma((len(pieces),)),
            dma((1,)),
            dma((len(pieces),)),
            dma((len(pieces),)),
            dma((3, len(parts))),
            dma((6,)),
        ],
        compiler_params=pltpu.CompilerParams(
            collective_id=0, has_side_effects=True, vmem_limit_bytes=66000000
        ),
        name="decode_layer",
    )(
        lengths,
        routes,
        gate_logits,
        hidden_in,
        norm_gain.reshape(1, width),
        queries,
        new_keys,
        new_values,
        cache_keys,
        cache_values,
        w_gate,
        w_up,
        w_down,
    )


def solution(mesh):
    in_specs = (
        P(None, ("grp", "dp"), None),
        P(),
        P(None, ("grp", "dp"), None),
        P(None, ("grp", "dp"), None),
        P(None, ("grp", "dp"), None),
        P(("grp", "dp"), None, None),
        P(("grp", "dp"), None, None),
        P(("grp", "dp")),
        P(None, ("grp", "dp"), None),
        P(None, ("grp", "dp"), None),
        P("dp", None),
        P("dp", None),
        P("dp", None),
    )
    out_specs = P(None, ("grp", "dp"), None)
    return jax.shard_map(
        per_device, mesh=mesh, in_specs=in_specs, out_specs=out_specs, check_vma=False
    )
```

```python
import functools

import jax
import jax.numpy as jnp
from jax import lax
from jax.experimental import pallas as pl
from jax.experimental.pallas import tpu as pltpu
from jax.sharding import PartitionSpec as P

HEAD_DIM = 128
EXPERTS = 4
PAD = 16
MESH = pl.DeviceIdType.MESH
F32 = jnp.float32
BF16 = jnp.bfloat16
NEG = -1e30
PARTS = ((2, False), (1, False), (1, True), (1, True), (1, True), (1, True), (1, True))
ROWS_BY_ROWS = (((1,), (1,)), ((), ()))
COLS_BY_ROWS = (((0,), (0,)), ((), ()))


def kernel(
    n,
    pieces,
    parts,
    lengths_hbm,
    routes_hbm,
    logits_hbm,
    hidden_hbm,
    gain_hbm,
    q_hbm,
    nk_hbm,
    nv_hbm,
    ck_hbm,
    cv_hbm,
    wg_hbm,
    wu_hbm,
    wd_hbm,
    out_ref,
    lengths_ref,
    routes_ref,
    logits_ref,
    hidden_ref,
    gain_ref,
    q_ref,
    nk_ref,
    nv_ref,
    kvbuf,
    wgu,
    wd,
    qs,
    bias,
    carried,
    blocks,
    xs,
    xb,
    ssq,
    acc_g,
    acc_u,
    act,
    part,
    s1,
    r1,
    s2,
    r2,
    s3,
    r3,
    s4,
    r4,
    sem_in,
    sem_kv,
    sem_gu,
    sem_d,
    sem_a,
    sem_c,
    sem_r,
    sem_s,
):
    new, docs, width = hidden_ref.shape
    tokens = new * docs
    cache_len, kv_width = ck_hbm.shape[1], ck_hbm.shape[2]
    kv_heads = kv_width // HEAD_DIM
    group = width // kv_width
    hidden = wg_hbm.shape[0]
    pair = 2
    nc = kv_heads // pair
    ck = width // nc
    nk = len(parts)
    relayed = [k for k, (_, _, direct) in enumerate(parts) if not direct]
    straight = [k for k, (_, _, direct) in enumerate(parts) if direct]
    quads = n // 4
    rows = n * tokens
    half = rows // 2
    score_scale = HEAD_DIM ** (-0.5)

    grp, me = lax.axis_index("grp"), lax.axis_index("dp")
    core = lax.rem(me, 2)
    xbit = lax.rem(me // 2, 2)
    quad = me // 4
    core_dev = (grp, me + 1 - 2 * core)
    x_dev = (grp, me + 2 - 4 * xbit)

    def opposite(x, d):
        at_x = xbit if x == 0 else 1 - xbit
        return (grp, lax.rem(quad + d, quads) * 4 + at_x * 2 + 1 - core)

    def back(d):
        return (quads - d) % quads

    order = [d for i in range(quads // 2, 0, -1) for d in dict.fromkeys([i, quads - i])] + [0]
    chips = [(x, d) for d in order for x in (1, 0)]
    barrier = pltpu.get_barrier_semaphore()
    for dev in [opposite(x, d) for x, d in chips] + [x_dev]:
        pl.semaphore_signal(barrier, inc=1, device_id=dev, device_id_type=MESH)

    smalls = [
        (q_hbm, q_ref),
        (nk_hbm, nk_ref),
        (nv_hbm, nv_ref),
        (lengths_hbm, lengths_ref),
        (hidden_hbm, hidden_ref),
        (gain_hbm, gain_ref),
        (routes_hbm, routes_ref),
        (logits_hbm, logits_ref),
    ]
    small_copies = [
        pltpu.make_async_copy(src, dst, sem_in.at[i]) for i, (src, dst) in enumerate(smalls)
    ]

    def lanes_of(c):
        return pl.ds(c * pair * HEAD_DIM, pair * HEAD_DIM)

    def cache_rows(c):
        return kvbuf.at[:, :, pl.ds(0, cache_len), lanes_of(c)]

    def cache_copies(c):
        return [
            pltpu.make_async_copy(src.at[:, :, lanes_of(c)], cache_rows(c).at[i], sem_kv.at[c])
            for i, src in enumerate((ck_hbm, cv_hbm))
        ]

    for copy in small_copies[:5] + cache_copies(0) + small_copies[5:]:
        copy.start()
    for c in range(1, nc):
        for copy in cache_copies(c):
            copy.start()

    def start_weights():
        for p, (at, size, _) in enumerate(pieces):
            for i, src in enumerate((wg_hbm, wu_hbm)):
                lanes = pl.ds(at, size)
                pltpu.make_async_copy(src.at[:, lanes], wgu.at[i, :, lanes], sem_gu.at[p]).start()
        pltpu.make_async_copy(wd_hbm, wd, sem_d.at[0]).start()

    with jax.named_scope("inwait"):
        for copy in small_copies[:5]:
            copy.wait()
    for t in range(new):
        q32 = q_ref[t].astype(F32)
        for head in range(kv_heads * group):
            qs[head * tokens + t * docs : head * tokens + (t + 1) * docs, :] = q32[
                :, head * HEAD_DIM : (head + 1) * HEAD_DIM
            ]
        carried[t * docs : (t + 1) * docs, :] = hidden_ref[t].astype(F32)
    extra = lax.broadcasted_iota(jnp.int32, (PAD, kv_width), 0)
    for i, src in enumerate((nk_ref, nv_ref)):
        for d in range(docs):
            value = jnp.zeros((PAD, kv_width), F32)
            for u in range(new):
                value = jnp.where(extra == u, src[u, d : d + 1].astype(F32), value)
            kvbuf[i, d, cache_len : cache_len + PAD, :] = value.astype(BF16)
    prow = pair * group * tokens
    row = lax.broadcasted_iota(jnp.int32, (prow, cache_len + PAD), 0)
    col = lax.broadcasted_iota(jnp.int32, (prow, cache_len + PAD), 1)
    row_doc = lax.rem(row, docs)
    row_new = lax.rem(row, tokens) // docs
    limit = jnp.zeros_like(row)
    for d in range(docs):
        limit = jnp.where(row_doc == d, lengths_ref[d], limit)
    keep = (col < limit) | ((col >= cache_len) & (col - cache_len <= row_new))
    keep = jnp.logical_and(keep, (col < cache_len) | (col < cache_len + new))
    bias[...] = jnp.where(keep, 0.0, NEG)

    def block_copy(p, src, dst, count, send_sem, recv_sem, dev):
        lanes = pl.ds(pieces[p][0], pieces[p][1])
        return pltpu.make_async_remote_copy(
            src_ref=blocks.at[pl.ds(src, count), :, lanes],
            dst_ref=blocks.at[pl.ds(dst, count), :, lanes],
            send_sem=sem_s.at[send_sem],
            recv_sem=recv_sem.at[p],
            device_id=dev,
            device_id_type=MESH,
        )

    mine = core * 2 * quads
    theirs = (1 - core) * 2 * quads

    def scores_of(c):
        zeros = jnp.zeros((group * tokens, HEAD_DIM), F32)
        lines = []
        for i in range(pair):
            h = c * pair + i
            q = qs[h * group * tokens : (h + 1) * group * tokens, :]
            lines.append(jnp.concatenate([zeros] * i + [q] + [zeros] * (pair - 1 - i), axis=1))
        q = jnp.concatenate(lines, axis=0).astype(BF16)
        lanes = slice(c * pair * HEAD_DIM, (c + 1) * pair * HEAD_DIM)
        value = None
        for d in range(docs):
            s = lax.dot_general(
                q, kvbuf[0, d, :, lanes], ROWS_BY_ROWS, preferred_element_type=F32
            )
            value = s if d == 0 else jnp.where(row_doc == d, s, value)
        return value

    def context_of(c, value):
        value = value * score_scale + bias[...]
        e = jnp.exp(value - jnp.max(value, axis=1, keepdims=True))
        p = e * (1.0 / jnp.sum(e, axis=1, keepdims=True))
        lanes = slice(c * pair * HEAD_DIM, (c + 1) * pair * HEAD_DIM)
        result = None
        for d in range(docs):
            r = jnp.dot(
                jnp.where(row_doc == d, p, 0.0).astype(BF16),
                kvbuf[1, d, :, lanes],
                preferred_element_type=F32,
            )
            result = r if d == 0 else result + r
        pieces = []
        for i in range(pair):
            for g in range(group):
                at = (i * group + g) * tokens
                pieces.append(result[at : at + tokens, i * HEAD_DIM : (i + 1) * HEAD_DIM])
        return jnp.concatenate(pieces, axis=1)

    def wait_cache(c):
        with jax.named_scope(f"kv{c}"):
            pltpu.make_async_copy(cache_rows(c), cache_rows(c), sem_kv.at[c]).wait()

    def attend(c, value):
        with jax.named_scope(f"attn{c}"):
            lanes = slice(c * ck, (c + 1) * ck)
            car = carried[:, lanes] + context_of(c, value)
            carried[:, lanes] = car
            blocks[mine, :, lanes] = car.astype(BF16)

    def send_chunk(c):
        for p, (_, _, chunk) in enumerate(pieces):
            if chunk == c:
                for x, d in chips:
                    slot = mine + x * quads + back(d)
                    block_copy(p, mine, slot, 1, 0, sem_a, opposite(x, d)).start()

    wait_cache(0)
    attend(0, scores_of(0))
    start_weights()
    with jax.named_scope("bar"):
        pl.semaphore_wait(barrier, 2 * quads + 1)
    send_chunk(0)
    for c in range(1, nc):
        wait_cache(c)
    with jax.named_scope("scores1"):
        values = [scores_of(c) for c in range(1, nc)]
    for c in range(1, nc):
        attend(c, values[c - 1])
        send_chunk(c)
    for copy in small_copies[5:]:
        copy.wait()

    def forward(p):
        with jax.named_scope(f"A{p}"):
            block_copy(p, theirs, theirs, 2 * quads, 0, sem_a, core_dev).wait_recv()
            block_copy(p, theirs + 1, theirs + 1, 2 * quads - 1, 1, sem_c, core_dev).start()

    def gather(p):
        at, size, _ = pieces[p]
        lanes = slice(at, at + size)
        with jax.named_scope(f"C{p}"):
            block_copy(p, mine + 1, mine + 1, 2 * quads - 1, 1, sem_c, core_dev).wait_recv()
        for b in range(n):
            xs[b * tokens : (b + 1) * tokens, 0:size] = blocks[b, :, lanes].astype(F32)
        value = xs[:, 0:size]
        square = value * value
        total = square[:, 0:HEAD_DIM]
        for i in range(1, size // HEAD_DIM):
            total = total + square[:, i * HEAD_DIM : (i + 1) * HEAD_DIM]
        ssq[...] = total if p == 0 else ssq[...] + total
        xb[:, lanes] = (value * gain_ref[:, lanes]).astype(BF16)

    nh = 2
    hc = hidden // nh

    def gate_up(p, j, scale):
        rows_at = slice(j * hc, (j + 1) * hc)
        lanes = slice(pieces[p][0], pieces[p][0] + pieces[p][1])
        x = xb[:, lanes]
        g = lax.dot_general(wgu[0, rows_at, lanes], x, ROWS_BY_ROWS, preferred_element_type=F32)
        u = lax.dot_general(wgu[1, rows_at, lanes], x, ROWS_BY_ROWS, preferred_element_type=F32)
        if p > 0:
            g = g + acc_g[rows_at, :]
            u = u + acc_u[rows_at, :]
        if p < len(pieces) - 1:
            acc_g[rows_at, :] = g
            acc_u[rows_at, :] = u
        else:
            g = g * scale
            act[rows_at, :] = (g * jax.nn.sigmoid(g) * (u * scale)).astype(BF16)

    for p in range(2):
        forward(p)
    for p, (at, size, _) in enumerate(pieces):
        gather(p)
        scale = None
        if p == len(pieces) - 1:
            total = jnp.sum(jnp.transpose(ssq[...]), axis=0, keepdims=True)
            scale = lax.rsqrt(total / width + 1e-05)
        with jax.named_scope(f"guwait{p}"):
            ref = wgu.at[:, :, pl.ds(at, size)]
            pltpu.make_async_copy(ref, ref, sem_gu.at[p]).wait()
        for j in range(nh):
            with jax.named_scope(f"gu{p}"):
                gate_up(p, j, scale)
        if p + 2 < len(pieces):
            forward(p + 2)

    def pair_copy(src, dst, stage, k, dev):
        return pltpu.make_async_remote_copy(
            src_ref=src,
            dst_ref=dst,
            send_sem=sem_s.at[2 + stage],
            recv_sem=sem_r.at[min(stage, 2), k],
            device_id=dev,
            device_id_type=MESH,
        )

    def lanes_at(k):
        return pl.ds(parts[k][0], parts[k][1])

    copy_1 = [
        pair_copy(s1.at[core, :, lanes_at(k)], r1.at[:, lanes_at(k)], 0, k, core_dev)
        for k in range(nk)
    ]
    copy_2 = {
        k: pair_copy(s2.at[1, :, lanes_at(k)], r2.at[:, lanes_at(k)], 1, k, x_dev)
        for k in relayed
    }

    def sends_3(k):
        lanes = lanes_at(k)
        return [
            pair_copy(s3.at[d, :, lanes], r3.at[back(d), :, lanes], 2, k, opposite(0, d))
            for d in order
        ]

    def sends_4(k):
        lanes = lanes_at(k)
        return [
            pair_copy(
                s4.at[x * quads + d, :, lanes],
                r4.at[x * quads + back(d), :, lanes],
                3,
                k,
                opposite(x, d),
            )
            for x, d in chips
        ]

    def start_1(k):
        at, size, _ = parts[k]
        lanes = slice(at, at + size)
        with jax.named_scope(f"down{k}"):
            value = lax.dot_general(act[...], wd[:, lanes], COLS_BY_ROWS, preferred_element_type=F32)
            s1[0, :, lanes] = value[:half].astype(BF16)
            s1[1, :, lanes] = value[half:].astype(BF16)
        copy_1[k].start()

    def start_2(k):
        at, size, direct = parts[k]
        lanes = slice(at, at + size)
        with jax.named_scope(f"r1wait{k}"):
            copy_1[k].wait_recv()
        value = s1[1 - core, :, lanes].astype(F32) + r1[:, lanes].astype(F32)
        if direct:
            for i in range(2 * quads):
                s4[i, :, lanes] = value[i * tokens : (i + 1) * tokens].astype(BF16)
            for copy in sends_4(k):
                copy.start()
        else:
            value = value.astype(BF16)
            s2[0, :, lanes] = value[: half // 2]
            s2[1, :, lanes] = value[half // 2 :]
            copy_2[k].start()

    def start_3(k):
        at, size, _ = parts[k]
        lanes = slice(at, at + size)
        with jax.named_scope(f"r2wait{k}"):
            copy_2[k].wait_recv()
        part[:, 0:size] = s2[0, :, lanes].astype(F32) + r2[:, lanes].astype(F32)
        for q in range(quads):
            s3[q, :, lanes] = part[q * tokens : (q + 1) * tokens, 0:size].astype(BF16)
        for copy in sends_3(k):
            copy.start()

    token = lax.broadcasted_iota(jnp.int32, (tokens, 1), 0)
    margin = jnp.zeros((tokens, 1), F32)
    first = jnp.zeros((tokens, 1), jnp.int32)
    second = jnp.zeros((tokens, 1), jnp.int32)
    for t in range(new):
        for d in range(docs):
            here = token == t * docs + d
            margin = jnp.where(here, logits_ref[t, d, 0] - logits_ref[t, d, 1], margin)
            first = jnp.where(here, routes_ref[t, d, 0], first)
            second = jnp.where(here, routes_ref[t, d, 1], second)
    share_a = jax.nn.sigmoid(margin)
    share_b = 1.0 - share_a
    share = []
    for d in range(quads):
        e = lax.rem(quad + d, quads) // (quads // EXPERTS)
        share.append(jnp.where(first == e, share_a, 0.0) + jnp.where(second == e, share_b, 0.0))

    def finish(k):
        at, size, direct = parts[k]
        lanes = slice(at, at + size)
        with jax.named_scope(f"r3wait{k}"):
            src, dst = (s4, r4) if direct else (s3, r3)
            pair_copy(
                src.at[:, :, lanes_at(k)], dst.at[:, :, lanes_at(k)], 3 if direct else 2, k, core_dev
            ).wait_recv()
        acc = carried[:, lanes]
        for d in range(quads):
            if direct:
                value = r4[d, :, lanes].astype(F32) + r4[quads + d, :, lanes].astype(F32)
            else:
                value = r3[d, :, lanes].astype(F32)
            acc = acc + share[d] * value
        for t in range(new):
            out_ref[t, :, lanes] = acc[t * docs : (t + 1) * docs].astype(out_ref.dtype)

    with jax.named_scope("dwait"):
        pltpu.make_async_copy(wd_hbm, wd, sem_d.at[0]).wait()
    lag = min(2, nk)
    for k in range(nk):
        start_1(k)
        if k >= lag:
            start_2(k - lag)
    for k in range(nk - lag, nk):
        start_2(k)
    for k in relayed:
        start_3(k)
    for k in range(nk):
        finish(k)

    def span(indices):
        at = parts[indices[0]][0]
        return pl.ds(at, parts[indices[-1]][0] + parts[indices[-1]][1] - at)

    with jax.named_scope("sends"):
        sent = [blocks.at[pl.ds(0, 2 * quads)], blocks.at[pl.ds(0, 2 * quads - 1)], r1]
        sent += [r2.at[:, span(relayed)], s3.at[:, :, span(relayed)], s4.at[:, :, span(straight)]]
        for i, ref in enumerate(sent):
            pltpu.make_async_remote_copy(
                src_ref=ref,
                dst_ref=ref,
                send_sem=sem_s.at[i],
                recv_sem=sem_s.at[i],
                device_id=core_dev,
                device_id_type=MESH,
            ).wait_send()


def per_device(
    hidden_in,
    norm_gain,
    queries,
    new_keys,
    new_values,
    cache_keys,
    cache_values,
    lengths,
    routes,
    gate_logits,
    w_gate,
    w_up,
    w_down,
):
    n = lax.axis_size("dp")
    new, docs, width = hidden_in.shape
    tokens = new * docs
    rows = n * tokens
    hidden = w_gate.shape[0]
    cache_len, kv_width = cache_keys.shape[1:]
    kv_heads = kv_width // HEAD_DIM
    group = width // kv_width
    quads = n // 4
    chunk = 2 * HEAD_DIM * group
    pieces = [(0, chunk // 2, 0), (chunk // 2, chunk // 2, 0)]
    pieces += [(c * chunk, chunk, c) for c in range(1, width // chunk)]
    parts, at = [], 0
    for size, direct in PARTS:
        parts.append((at * width // 8, size * width // 8, direct))
        at += size
    vmem = pl.BlockSpec(memory_space=pltpu.VMEM)
    hbm = pl.BlockSpec(memory_space=pl.ANY)
    dma = pltpu.SemaphoreType.DMA
    return pl.pallas_call(
        functools.partial(kernel, n, pieces, parts),
        out_shape=pltpu.VMEM(hidden_in.shape, BF16),
        in_specs=[hbm] * 13,
        out_specs=vmem,
        scratch_shapes=[
            pltpu.SMEM(lengths.shape, jnp.int32),
            pltpu.SMEM(routes.shape, jnp.int32),
            pltpu.SMEM(gate_logits.shape, F32),
            pltpu.VMEM(hidden_in.shape, BF16),
            pltpu.VMEM((1, width), F32),
            pltpu.VMEM(queries.shape, BF16),
            pltpu.VMEM(new_keys.shape, BF16),
            pltpu.VMEM(new_values.shape, BF16),
            pltpu.VMEM((2, docs, cache_len + PAD, kv_width), BF16),
            pltpu.VMEM((2, hidden, width), BF16),
            pltpu.VMEM((hidden, width), BF16),
            pltpu.VMEM((kv_heads * group * tokens, HEAD_DIM), F32),
            pltpu.VMEM((2 * group * tokens, cache_len + PAD), F32),
            pltpu.VMEM((tokens, width), F32),
            pltpu.VMEM((n, tokens, width), BF16),
            pltpu.VMEM((rows, chunk), F32),
            pltpu.VMEM((rows, width), BF16),
            pltpu.VMEM((rows, HEAD_DIM), F32),
            pltpu.VMEM((hidden, rows), F32),
            pltpu.VMEM((hidden, rows), F32),
            pltpu.VMEM((hidden, rows), BF16),
            pltpu.VMEM((rows // 4, chunk), F32),
            pltpu.VMEM((2, rows // 2, width), BF16),
            pltpu.VMEM((rows // 2, width), BF16),
            pltpu.VMEM((2, rows // 4, width), BF16),
            pltpu.VMEM((rows // 4, width), BF16),
            pltpu.VMEM((quads, tokens, width), BF16),
            pltpu.VMEM((quads, tokens, width), BF16),
            pltpu.VMEM((2 * quads, tokens, width), BF16),
            pltpu.VMEM((2 * quads, tokens, width), BF16),
            dma((8,)),
            dma((kv_heads // 2,)),
            dma((len(pieces),)),
            dma((1,)),
            dma((len(pieces),)),
            dma((len(pieces),)),
            dma((3, len(parts))),
            dma((6,)),
        ],
        compiler_params=pltpu.CompilerParams(
            collective_id=0, has_side_effects=True, vmem_limit_bytes=66000000
        ),
        name="decode_layer",
    )(
        lengths,
        routes,
        gate_logits,
        hidden_in,
        norm_gain.reshape(1, width),
        queries,
        new_keys,
        new_values,
        cache_keys,
        cache_values,
        w_gate,
        w_up,
        w_down,
    )


def solution(mesh):
    in_specs = (
        P(None, ("grp", "dp"), None),
        P(),
        P(None, ("grp", "dp"), None),
        P(None, ("grp", "dp"), None),
        P(None, ("grp", "dp"), None),
        P(("grp", "dp"), None, None),
        P(("grp", "dp"), None, None),
        P(("grp", "dp")),
        P(None, ("grp", "dp"), None),
        P(None, ("grp", "dp"), None),
        P("dp", None),
        P("dp", None),
        P("dp", None),
    )
    out_specs = P(None, ("grp", "dp"), None)
    return jax.shard_map(
        per_device, mesh=mesh, in_specs=in_specs, out_specs=out_specs, check_vma=False
    )
```

```python
import functools

import jax
import jax.numpy as jnp
from jax import lax
from jax.experimental import pallas as pl
from jax.experimental.pallas import tpu as pltpu
from jax.sharding import PartitionSpec as P

HEAD_DIM = 128
EXPERTS = 4
PAD = 16
MESH = pl.DeviceIdType.MESH
F32 = jnp.float32
BF16 = jnp.bfloat16
NEG = -1e30
PARTS = ((2, False), (1, True), (1, True), (1, True), (1, True), (1, True), (1, True))
ROWS_BY_ROWS = (((1,), (1,)), ((), ()))
COLS_BY_ROWS = (((0,), (0,)), ((), ()))


def kernel(
    n,
    pieces,
    parts,
    lengths_hbm,
    routes_hbm,
    logits_hbm,
    hidden_hbm,
    gain_hbm,
    q_hbm,
    nk_hbm,
    nv_hbm,
    ck_hbm,
    cv_hbm,
    wg_hbm,
    wu_hbm,
    wd_hbm,
    out_ref,
    lengths_ref,
    routes_ref,
    logits_ref,
    hidden_ref,
    gain_ref,
    q_ref,
    nk_ref,
    nv_ref,
    kvbuf,
    wgu,
    wd,
    qs,
    bias,
    carried,
    blocks,
    xs,
    xb,
    ssq,
    acc_g,
    acc_u,
    act,
    part,
    s1,
    r1,
    s2,
    r2,
    s3,
    r3,
    s4,
    r4,
    sem_in,
    sem_kv,
    sem_gu,
    sem_d,
    sem_a,
    sem_c,
    sem_r,
    sem_s,
):
    new, docs, width = hidden_ref.shape
    tokens = new * docs
    cache_len, kv_width = ck_hbm.shape[1], ck_hbm.shape[2]
    kv_heads = kv_width // HEAD_DIM
    group = width // kv_width
    hidden = wg_hbm.shape[0]
    pair = 2
    nc = kv_heads // pair
    ck = width // nc
    nk = len(parts)
    relayed = [k for k, (_, _, direct) in enumerate(parts) if not direct]
    straight = [k for k, (_, _, direct) in enumerate(parts) if direct]
    quads = n // 4
    rows = n * tokens
    half = rows // 2
    score_scale = HEAD_DIM ** (-0.5)

    grp, me = lax.axis_index("grp"), lax.axis_index("dp")
    core = lax.rem(me, 2)
    xbit = lax.rem(me // 2, 2)
    quad = me // 4
    core_dev = (grp, me + 1 - 2 * core)
    x_dev = (grp, me + 2 - 4 * xbit)

    def opposite(x, d):
        at_x = xbit if x == 0 else 1 - xbit
        return (grp, lax.rem(quad + d, quads) * 4 + at_x * 2 + 1 - core)

    def back(d):
        return (quads - d) % quads

    order = [d for i in range(quads // 2, 0, -1) for d in dict.fromkeys([i, quads - i])] + [0]
    chips = [(x, d) for d in order for x in (1, 0)]
    barrier = pltpu.get_barrier_semaphore()
    for dev in [opposite(x, d) for x, d in chips] + [x_dev]:
        pl.semaphore_signal(barrier, inc=1, device_id=dev, device_id_type=MESH)

    smalls = [
        (q_hbm, q_ref),
        (nk_hbm, nk_ref),
        (nv_hbm, nv_ref),
        (lengths_hbm, lengths_ref),
        (hidden_hbm, hidden_ref),
        (gain_hbm, gain_ref),
        (routes_hbm, routes_ref),
        (logits_hbm, logits_ref),
    ]
    small_copies = [
        pltpu.make_async_copy(src, dst, sem_in.at[i]) for i, (src, dst) in enumerate(smalls)
    ]

    def lanes_of(c):
        return pl.ds(c * pair * HEAD_DIM, pair * HEAD_DIM)

    def cache_rows(c):
        return kvbuf.at[:, :, pl.ds(0, cache_len), lanes_of(c)]

    def cache_copies(c):
        return [
            pltpu.make_async_copy(src.at[:, :, lanes_of(c)], cache_rows(c).at[i], sem_kv.at[c])
            for i, src in enumerate((ck_hbm, cv_hbm))
        ]

    for copy in cache_copies(0) + small_copies:
        copy.start()
    for c in range(1, nc):
        for copy in cache_copies(c):
            copy.start()

    def start_weights():
        for p, (at, size, _) in enumerate(pieces):
            for i, src in enumerate((wg_hbm, wu_hbm)):
                lanes = pl.ds(at, size)
                pltpu.make_async_copy(src.at[:, lanes], wgu.at[i, :, lanes], sem_gu.at[p]).start()
        pltpu.make_async_copy(wd_hbm, wd, sem_d.at[0]).start()

    with jax.named_scope("inwait"):
        for copy in small_copies[:5]:
            copy.wait()
    for t in range(new):
        q32 = q_ref[t].astype(F32)
        for head in range(kv_heads * group):
            qs[head * tokens + t * docs : head * tokens + (t + 1) * docs, :] = q32[
                :, head * HEAD_DIM : (head + 1) * HEAD_DIM
            ]
        carried[t * docs : (t + 1) * docs, :] = hidden_ref[t].astype(F32)
    extra = lax.broadcasted_iota(jnp.int32, (PAD, kv_width), 0)
    for i, src in enumerate((nk_ref, nv_ref)):
        for d in range(docs):
            value = jnp.zeros((PAD, kv_width), F32)
            for u in range(new):
                value = jnp.where(extra == u, src[u, d : d + 1].astype(F32), value)
            kvbuf[i, d, cache_len : cache_len + PAD, :] = value.astype(BF16)
    prow = pair * group * tokens
    row = lax.broadcasted_iota(jnp.int32, (prow, cache_len + PAD), 0)
    col = lax.broadcasted_iota(jnp.int32, (prow, cache_len + PAD), 1)
    row_doc = lax.rem(row, docs)
    row_new = lax.rem(row, tokens) // docs
    limit = jnp.zeros_like(row)
    for d in range(docs):
        limit = jnp.where(row_doc == d, lengths_ref[d], limit)
    keep = (col < limit) | ((col >= cache_len) & (col - cache_len <= row_new))
    keep = jnp.logical_and(keep, (col < cache_len) | (col < cache_len + new))
    bias[...] = jnp.where(keep, 0.0, NEG)

    def block_copy(p, src, dst, count, send_sem, recv_sem, dev):
        lanes = pl.ds(pieces[p][0], pieces[p][1])
        return pltpu.make_async_remote_copy(
            src_ref=blocks.at[pl.ds(src, count), :, lanes],
            dst_ref=blocks.at[pl.ds(dst, count), :, lanes],
            send_sem=sem_s.at[send_sem],
            recv_sem=recv_sem.at[p],
            device_id=dev,
            device_id_type=MESH,
        )

    mine = core * 2 * quads
    theirs = (1 - core) * 2 * quads

    def scores_of(c):
        zeros = jnp.zeros((group * tokens, HEAD_DIM), F32)
        lines = []
        for i in range(pair):
            h = c * pair + i
            q = qs[h * group * tokens : (h + 1) * group * tokens, :]
            lines.append(jnp.concatenate([zeros] * i + [q] + [zeros] * (pair - 1 - i), axis=1))
        q = jnp.concatenate(lines, axis=0).astype(BF16)
        lanes = slice(c * pair * HEAD_DIM, (c + 1) * pair * HEAD_DIM)
        value = None
        for d in range(docs):
            s = lax.dot_general(
                q, kvbuf[0, d, :, lanes], ROWS_BY_ROWS, preferred_element_type=F32
            )
            value = s if d == 0 else jnp.where(row_doc == d, s, value)
        return value

    def context_of(c, value):
        value = value * score_scale + bias[...]
        e = jnp.exp(value - jnp.max(value, axis=1, keepdims=True))
        p = e * (1.0 / jnp.sum(e, axis=1, keepdims=True))
        lanes = slice(c * pair * HEAD_DIM, (c + 1) * pair * HEAD_DIM)
        result = None
        for d in range(docs):
            r = jnp.dot(
                jnp.where(row_doc == d, p, 0.0).astype(BF16),
                kvbuf[1, d, :, lanes],
                preferred_element_type=F32,
            )
            result = r if d == 0 else result + r
        pieces = []
        for i in range(pair):
            for g in range(group):
                at = (i * group + g) * tokens
                pieces.append(result[at : at + tokens, i * HEAD_DIM : (i + 1) * HEAD_DIM])
        return jnp.concatenate(pieces, axis=1)

    def wait_cache(c):
        with jax.named_scope(f"kv{c}"):
            pltpu.make_async_copy(cache_rows(c), cache_rows(c), sem_kv.at[c]).wait()

    def attend(c, value):
        with jax.named_scope(f"attn{c}"):
            lanes = slice(c * ck, (c + 1) * ck)
            car = carried[:, lanes] + context_of(c, value)
            carried[:, lanes] = car
            blocks[mine, :, lanes] = car.astype(BF16)

    def send_chunk(c):
        for p, (_, _, chunk) in enumerate(pieces):
            if chunk == c:
                for x, d in chips:
                    slot = mine + x * quads + back(d)
                    block_copy(p, mine, slot, 1, 0, sem_a, opposite(x, d)).start()

    wait_cache(0)
    attend(0, scores_of(0))
    start_weights()
    with jax.named_scope("bar"):
        pl.semaphore_wait(barrier, 2 * quads + 1)
    send_chunk(0)
    for c in range(1, nc):
        wait_cache(c)
    with jax.named_scope("scores1"):
        values = [scores_of(c) for c in range(1, nc)]
    for c in range(1, nc):
        attend(c, values[c - 1])
        send_chunk(c)
    for copy in small_copies[5:]:
        copy.wait()

    def forward(p):
        with jax.named_scope(f"A{p}"):
            block_copy(p, theirs, theirs, 2 * quads, 0, sem_a, core_dev).wait_recv()
            block_copy(p, theirs + 1, theirs + 1, 2 * quads - 1, 1, sem_c, core_dev).start()

    def gather(p):
        at, size, _ = pieces[p]
        lanes = slice(at, at + size)
        with jax.named_scope(f"C{p}"):
            block_copy(p, mine + 1, mine + 1, 2 * quads - 1, 1, sem_c, core_dev).wait_recv()
        for b in range(n):
            xs[b * tokens : (b + 1) * tokens, 0:size] = blocks[b, :, lanes].astype(F32)
        value = xs[:, 0:size]
        square = value * value
        total = square[:, 0:HEAD_DIM]
        for i in range(1, size // HEAD_DIM):
            total = total + square[:, i * HEAD_DIM : (i + 1) * HEAD_DIM]
        ssq[...] = total if p == 0 else ssq[...] + total
        xb[:, lanes] = (value * gain_ref[:, lanes]).astype(BF16)

    nh = 2
    hc = hidden // nh

    def gate_up(p, j, scale):
        rows_at = slice(j * hc, (j + 1) * hc)
        lanes = slice(pieces[p][0], pieces[p][0] + pieces[p][1])
        x = xb[:, lanes]
        g = lax.dot_general(wgu[0, rows_at, lanes], x, ROWS_BY_ROWS, preferred_element_type=F32)
        u = lax.dot_general(wgu[1, rows_at, lanes], x, ROWS_BY_ROWS, preferred_element_type=F32)
        if p > 0:
            g = g + acc_g[rows_at, :]
            u = u + acc_u[rows_at, :]
        if p < len(pieces) - 1:
            acc_g[rows_at, :] = g
            acc_u[rows_at, :] = u
        else:
            g = g * scale
            act[rows_at, :] = (g * jax.nn.sigmoid(g) * (u * scale)).astype(BF16)

    for p in range(2):
        forward(p)
    for p, (at, size, _) in enumerate(pieces):
        gather(p)
        scale = None
        if p == len(pieces) - 1:
            total = jnp.sum(jnp.transpose(ssq[...]), axis=0, keepdims=True)
            scale = lax.rsqrt(total / width + 1e-05)
        with jax.named_scope(f"guwait{p}"):
            ref = wgu.at[:, :, pl.ds(at, size)]
            pltpu.make_async_copy(ref, ref, sem_gu.at[p]).wait()
        for j in range(nh):
            with jax.named_scope(f"gu{p}"):
                gate_up(p, j, scale)
        if p + 2 < len(pieces):
            forward(p + 2)

    def pair_copy(src, dst, stage, k, dev):
        return pltpu.make_async_remote_copy(
            src_ref=src,
            dst_ref=dst,
            send_sem=sem_s.at[2 + stage],
            recv_sem=sem_r.at[(0, 2 * nk, nk, nk)[stage] + k],
            device_id=dev,
            device_id_type=MESH,
        )

    def lanes_at(k):
        return pl.ds(parts[k][0], parts[k][1])

    copy_1 = [
        pair_copy(s1.at[core, :, lanes_at(k)], r1.at[:, lanes_at(k)], 0, k, core_dev)
        for k in range(nk)
    ]
    copy_2 = {
        k: pair_copy(s2.at[1, :, lanes_at(k)], r2.at[:, lanes_at(k)], 1, k, x_dev)
        for k in relayed
    }

    def sends_3(k):
        lanes = lanes_at(k)
        return [
            pair_copy(s3.at[d, :, lanes], r3.at[back(d), :, lanes], 2, k, opposite(0, d))
            for d in order
        ]

    def sends_4(k):
        lanes = lanes_at(k)
        return [
            pair_copy(
                s4.at[x * quads + d, :, lanes],
                r4.at[x * quads + back(d), :, lanes],
                3,
                k,
                opposite(x, d),
            )
            for x, d in chips
        ]

    def start_1(k):
        at, size, _ = parts[k]
        lanes = slice(at, at + size)
        with jax.named_scope(f"down{k}"):
            value = lax.dot_general(act[...], wd[:, lanes], COLS_BY_ROWS, preferred_element_type=F32)
            s1[0, :, lanes] = value[:half].astype(BF16)
            s1[1, :, lanes] = value[half:].astype(BF16)
        copy_1[k].start()

    def start_2(k):
        at, size, direct = parts[k]
        lanes = slice(at, at + size)
        with jax.named_scope(f"r1wait{k}"):
            copy_1[k].wait_recv()
        value = s1[1 - core, :, lanes].astype(F32) + r1[:, lanes].astype(F32)
        if direct:
            for i in range(2 * quads):
                s4[i, :, lanes] = value[i * tokens : (i + 1) * tokens].astype(BF16)
            for copy in sends_4(k):
                copy.start()
        else:
            value = value.astype(BF16)
            s2[0, :, lanes] = value[: half // 2]
            s2[1, :, lanes] = value[half // 2 :]
            copy_2[k].start()

    def start_3(k):
        at, size, _ = parts[k]
        lanes = slice(at, at + size)
        with jax.named_scope(f"r2wait{k}"):
            copy_2[k].wait_recv()
        part[:, 0:size] = s2[0, :, lanes].astype(F32) + r2[:, lanes].astype(F32)
        for q in range(quads):
            s3[q, :, lanes] = part[q * tokens : (q + 1) * tokens, 0:size].astype(BF16)
        for copy in sends_3(k):
            copy.start()

    token = lax.broadcasted_iota(jnp.int32, (tokens, 1), 0)
    margin = jnp.zeros((tokens, 1), F32)
    first = jnp.zeros((tokens, 1), jnp.int32)
    second = jnp.zeros((tokens, 1), jnp.int32)
    for t in range(new):
        for d in range(docs):
            here = token == t * docs + d
            margin = jnp.where(here, logits_ref[t, d, 0] - logits_ref[t, d, 1], margin)
            first = jnp.where(here, routes_ref[t, d, 0], first)
            second = jnp.where(here, routes_ref[t, d, 1], second)
    share_a = jax.nn.sigmoid(margin)
    share_b = 1.0 - share_a
    share = []
    for d in range(quads):
        e = lax.rem(quad + d, quads) // (quads // EXPERTS)
        share.append(jnp.where(first == e, share_a, 0.0) + jnp.where(second == e, share_b, 0.0))

    def finish(k):
        at, size, direct = parts[k]
        lanes = slice(at, at + size)
        with jax.named_scope(f"r3wait{k}"):
            src, dst = (s4, r4) if direct else (s3, r3)
            pair_copy(
                src.at[:, :, lanes_at(k)], dst.at[:, :, lanes_at(k)], 3 if direct else 2, k, core_dev
            ).wait_recv()
        acc = carried[:, lanes]
        for d in range(quads):
            if direct:
                value = r4[d, :, lanes].astype(F32) + r4[quads + d, :, lanes].astype(F32)
            else:
                value = r3[d, :, lanes].astype(F32)
            acc = acc + share[d] * value
        for t in range(new):
            out_ref[t, :, lanes] = acc[t * docs : (t + 1) * docs].astype(out_ref.dtype)

    with jax.named_scope("dwait"):
        pltpu.make_async_copy(wd_hbm, wd, sem_d.at[0]).wait()
    lag = min(2, nk)
    for k in range(nk):
        start_1(k)
        if k >= lag:
            start_2(k - lag)
    for k in range(nk - lag, nk):
        start_2(k)
    for k in relayed:
        start_3(k)
    for k in straight + relayed:
        finish(k)

    def span(indices):
        at = parts[indices[0]][0]
        return pl.ds(at, parts[indices[-1]][0] + parts[indices[-1]][1] - at)

    with jax.named_scope("sends"):
        sent = [blocks.at[pl.ds(0, 2 * quads)], blocks.at[pl.ds(0, 2 * quads - 1)], r1]
        sent += [r2.at[:, span(relayed)], s3.at[:, :, span(relayed)], s4.at[:, :, span(straight)]]
        for i, ref in enumerate(sent):
            pltpu.make_async_remote_copy(
                src_ref=ref,
                dst_ref=ref,
                send_sem=sem_s.at[i],
                recv_sem=sem_s.at[i],
                device_id=core_dev,
                device_id_type=MESH,
            ).wait_send()


def per_device(
    hidden_in,
    norm_gain,
    queries,
    new_keys,
    new_values,
    cache_keys,
    cache_values,
    lengths,
    routes,
    gate_logits,
    w_gate,
    w_up,
    w_down,
):
    n = lax.axis_size("dp")
    new, docs, width = hidden_in.shape
    tokens = new * docs
    rows = n * tokens
    hidden = w_gate.shape[0]
    cache_len, kv_width = cache_keys.shape[1:]
    kv_heads = kv_width // HEAD_DIM
    group = width // kv_width
    quads = n // 4
    chunk = 2 * HEAD_DIM * group
    pieces = [(0, chunk // 2, 0), (chunk // 2, chunk // 2, 0)]
    pieces += [(c * chunk, chunk, c) for c in range(1, width // chunk)]
    parts, at = [], 0
    for size, direct in PARTS:
        parts.append((at * width // 8, size * width // 8, direct))
        at += size
    vmem = pl.BlockSpec(memory_space=pltpu.VMEM)
    hbm = pl.BlockSpec(memory_space=pl.ANY)
    dma = pltpu.SemaphoreType.DMA
    return pl.pallas_call(
        functools.partial(kernel, n, pieces, parts),
        out_shape=pltpu.VMEM(hidden_in.shape, BF16),
        in_specs=[hbm] * 13,
        out_specs=vmem,
        scratch_shapes=[
            pltpu.SMEM(lengths.shape, jnp.int32),
            pltpu.SMEM(routes.shape, jnp.int32),
            pltpu.SMEM(gate_logits.shape, F32),
            pltpu.VMEM(hidden_in.shape, BF16),
            pltpu.VMEM((1, width), F32),
            pltpu.VMEM(queries.shape, BF16),
            pltpu.VMEM(new_keys.shape, BF16),
            pltpu.VMEM(new_values.shape, BF16),
            pltpu.VMEM((2, docs, cache_len + PAD, kv_width), BF16),
            pltpu.VMEM((2, hidden, width), BF16),
            pltpu.VMEM((hidden, width), BF16),
            pltpu.VMEM((kv_heads * group * tokens, HEAD_DIM), F32),
            pltpu.VMEM((2 * group * tokens, cache_len + PAD), F32),
            pltpu.VMEM((tokens, width), F32),
            pltpu.VMEM((n, tokens, width), BF16),
            pltpu.VMEM((rows, chunk), F32),
            pltpu.VMEM((rows, width), BF16),
            pltpu.VMEM((rows, HEAD_DIM), F32),
            pltpu.VMEM((hidden, rows), F32),
            pltpu.VMEM((hidden, rows), F32),
            pltpu.VMEM((hidden, rows), BF16),
            pltpu.VMEM((rows // 4, chunk), F32),
            pltpu.VMEM((2, rows // 2, width), BF16),
            pltpu.VMEM((rows // 2, width), BF16),
            pltpu.VMEM((2, rows // 4, width), BF16),
            pltpu.VMEM((rows // 4, width), BF16),
            pltpu.VMEM((quads, tokens, width), BF16),
            pltpu.VMEM((quads, tokens, width), BF16),
            pltpu.VMEM((2 * quads, tokens, width), BF16),
            pltpu.VMEM((2 * quads, tokens, width), BF16),
            dma((8,)),
            dma((kv_heads // 2,)),
            dma((len(pieces),)),
            dma((1,)),
            dma((len(pieces),)),
            dma((len(pieces),)),
            dma((3 * len(parts) - sum(direct for _, _, direct in parts),)),
            dma((6,)),
        ],
        compiler_params=pltpu.CompilerParams(
            collective_id=0, has_side_effects=True, vmem_limit_bytes=66000000
        ),
        name="decode_layer",
    )(
        lengths,
        routes,
        gate_logits,
        hidden_in,
        norm_gain.reshape(1, width),
        queries,
        new_keys,
        new_values,
        cache_keys,
        cache_values,
        w_gate,
        w_up,
        w_down,
    )


def solution(mesh):
    in_specs = (
        P(None, ("grp", "dp"), None),
        P(),
        P(None, ("grp", "dp"), None),
        P(None, ("grp", "dp"), None),
        P(None, ("grp", "dp"), None),
        P(("grp", "dp"), None, None),
        P(("grp", "dp"), None, None),
        P(("grp", "dp")),
        P(None, ("grp", "dp"), None),
        P(None, ("grp", "dp"), None),
        P("dp", None),
        P("dp", None),
        P("dp", None),
    )
    out_specs = P(None, ("grp", "dp"), None)
    return jax.shard_map(
        per_device, mesh=mesh, in_specs=in_specs, out_specs=out_specs, check_vma=False
    )
```
